256 devices in a mesh: tensor: 8 (over z), expert: 2 (over core), dp: 16 (over y, x).
Axes of the slice: x: 4, y: 4, z: 8, core: 2. Of those that a mesh axis runs over, the one named last changes fastest.
Arguments:
- tokens: bfloat16 [4096, 2048], P(('expert', 'dp')), may hold values from -6 to 6
- tangent: bfloat16 [4096, 2048], P(('expert', 'dp')), may hold values from -6 to 6
- cotangent: bfloat16 [4096, 2048], P(('expert', 'dp')), may hold values from -0.59765625 to 0.59765625
- expert_ids: int32 [4096, 8], P(('expert', 'dp')), may hold values from 0 to 15, all different within a row; in each aligned block of 128 rows (0 to 127, 128 to 255, ...) at most 96 rows name the same one
- gates: float32 [4096, 8], P(('expert', 'dp')), may hold values from 0.1 to 1
- w_in: bfloat16 [16, 2, 768, 2048], P(('tensor', 'expert'), None, None, 'dp'), may hold values from -0.125 to 0.125
- v_in: bfloat16 [16, 2, 768, 2048], P(('tensor', 'expert'), None, None, 'dp'), may hold values from -0.125 to 0.125
- w_out: bfloat16 [16, 768, 2048], P(('tensor', 'expert'), None, 'dp'), may hold values from -0.21875 to 0.21875
- v_out: bfloat16 [16, 768, 2048], P(('tensor', 'expert'), None, 'dp'), may hold values from -0.21875 to 0.21875
Outputs:
- hvp_tokens: float32 [4096, 2048], P(('expert', 'dp'))
- hvp_in: float32 [16, 2, 768, 2048], P(('tensor', 'expert'), None, None, 'dp')
- hvp_out: float32 [16, 768, 2048], P(('tensor', 'expert'), None, 'dp')
The draws below stay inside these ranges and needn't reach their ends.
Inputs may be any that keep to these rules, and one draw needn't show every extreme that they name: `expert_ids`: each token names 8 different experts; among the tokens of one block of 128 no expert is named more than 96 times, and some expert reaches 96 in some blocks.
All inputs are finite; a program needn't handle non-finite values.
Results may differ from the reference program's by a relative error of at most 0.013.
Values may be sent and summed in bfloat16 or wider, within the bound.
No kernel may reach another device: no remote copies, remote signals or barrier semaphores. Data moves between devices by JAX's collectives and lax.ppermute only.
A program may use at most 128 MiB of HBM per device.

```python
import math
import jax
import jax.numpy as jnp
import numpy as np
from jax import lax

D = 2048
FF = 768
TOPK = 8
TOK_DEV = 128
EXPERTS = 16
CAP = 96
TOKENS = 4096
N_EXPERT = 2
N_DP = 16


def level_of(rng, extent, pieces, least, high):
    def one(axis_at, blocks):
        draws = jax.random.uniform(jax.random.fold_in(jax.random.fold_in(rng, 6), axis_at), (blocks,), jnp.float32, least / len(pieces), high / len(pieces))
        return jnp.repeat(jnp.exp(draws), extent[axis_at] // blocks).reshape((-1,) + (1,) * (len(extent) - axis_at - 1))

    level = one(*pieces[0])
    for cut in pieces[1:]:
        level = level * one(*cut)
    return level


def routed_block(rng, own, number, rows, number_of, top, reach, slope):
    order = jax.random.permutation(rng, number_of)
    heavy_load, ordinary = shares(number_of, rows * top, reach, slope, True), shares(number_of, rows * top, reach, slope, False)
    places = jnp.arange(number_of)

    def named(tallies, turn):
        used = int((tallies > 0).sum())
        fixed = max(1, used // 4)
        passed = fixed + (places - fixed + turn * (used - fixed)) % max(1, number_of - fixed)
        return jnp.zeros((number_of,), jnp.int32).at[order[jnp.where(places < fixed, places, passed)]].set(jnp.asarray(tallies, jnp.int32))

    tallies = jnp.where(number % 4 == 0, named(heavy_load, number // 4), named(ordinary, number - number // 4 - 1))
    mixed = jax.random.permutation(jax.random.fold_in(own, 3), number_of)
    source_of, receiver = mixed[0:number_of // 2 * 2:2], mixed[1:number_of // 2 * 2:2]
    room = jnp.minimum(tallies[source_of] - 1, reach - tallies[receiver]) // 2
    room = jnp.where((source_of == order[0]) | (receiver == order[0]) | (tallies[receiver] == 0), 0, jnp.maximum(room, 0))
    passed = jax.random.randint(jax.random.fold_in(own, 4), (number_of // 2,), 0, 1 << 20) % (room + 1)
    tallies = tallies.at[source_of].add(-passed).at[receiver].add(passed)
    items = jnp.searchsorted(jnp.cumsum(tallies), jnp.arange(rows * top), side="right").astype(jnp.int32)
    table = items.reshape(top, rows).T
    table = table[jax.random.permutation(jax.random.fold_in(own, 1), rows)]
    turn = jax.random.randint(jax.random.fold_in(own, 2), (rows, 1), 0, top)
    return jnp.take_along_axis(table, (jnp.arange(top)[None, :] + turn) % top, axis=1)


def shares(amount, total, reach, lean, full):
    portions = [(1 << 20) // math.isqrt(standing ** lean) + 1 for standing in range(1, amount + 1)]
    largest = reach if full else min(reach, max(-(-total // amount), total * portions[0] // sum(portions)))
    least = 1 if total - largest >= amount - 1 else 0
    holding, rest = [largest] + [least] * (amount - 1), total - largest - least * (amount - 1)
    while rest > 0:
        free = [i for i in range(1, amount) if holding[i] < largest] or [i for i in range(1, amount) if holding[i] < reach]
        mass, budget = sum([portions[i] for i in free]), rest
        for i in free:
            addition = min(reach - holding[i], max(1, budget * portions[i] // mass), rest)
            holding[i] = holding[i] + addition
            rest = rest - addition
    return np.array(holding)


def scatter_about(rng, extent, width, bound, split=(), kind=jnp.bfloat16):
    factor_of = level_of(rng, extent, split, -0.22, 0.18) if split else 1.0
    entries = jax.random.normal(rng, extent, jnp.float32) * width * factor_of
    return jnp.minimum(jnp.maximum(entries, -bound), bound).astype(kind)


def setup_inputs(seed: int = 0) -> dict:
    key_of = jax.random.split(jax.random.key(seed), 10)
    tokens = scatter_about(key_of[0], (TOKENS, D), 1.0, 6.0, ((0, 32),))
    tangent = scatter_about(key_of[1], (TOKENS, D), 1.0, 6.0, ((0, 32),))
    cotangent = scatter_about(key_of[2], (TOKENS, D), 0.1, 0.59765625, ((0, 32),))
    expert_ids_keys = jax.random.split(jax.random.fold_in(key_of[3], 1), TOKENS // TOK_DEV)
    expert_ids_turns = jax.random.permutation(jax.random.fold_in(key_of[3], 3), TOKENS // TOK_DEV)
    expert_ids = jax.vmap(lambda own, number: routed_block(jax.random.fold_in(key_of[3], 2), own, number, TOK_DEV, EXPERTS, TOPK, CAP, 2))(expert_ids_keys, expert_ids_turns).reshape((TOKENS, TOPK))
    gates = jnp.clip(jnp.exp(math.log(1.0) - 2.3025851 * jax.random.uniform(key_of[4], (TOKENS, TOPK), jnp.float32) ** level_of(key_of[4], (TOKENS, TOPK), ((0, 32),), -0.2, 0.2)), 0.1, 1.0)
    w_in = scatter_about(key_of[5], (EXPERTS, 2, FF, D), D ** -0.5, 0.125, ((0, 16), (3, 16)))
    v_in = scatter_about(key_of[6], (EXPERTS, 2, FF, D), D ** -0.5, 0.125, ((0, 16), (3, 16)))
    w_out = scatter_about(key_of[7], (EXPERTS, FF, D), FF ** -0.5, 0.21875, ((0, 16), (2, 16)))
    v_out = scatter_about(key_of[8], (EXPERTS, FF, D), FF ** -0.5, 0.21875, ((0, 16), (2, 16)))
    return {"tokens": tokens, "tangent": tangent, "cotangent": cotangent, "expert_ids": expert_ids, "gates": gates, "w_in": w_in, "v_in": v_in, "w_out": w_out, "v_out": v_out}


def rounded(value):
    return lax.optimization_barrier(value.astype(jnp.bfloat16)).astype(jnp.float32)


def reference(tokens, tangent, cotangent, expert_ids, gates, w_in, v_in, w_out, v_out):
    blocks = N_EXPERT * N_DP
    pairs = TOK_DEV * TOPK
    picks = expert_ids.reshape(blocks, pairs).astype(jnp.int32)
    onehot = (picks[:, :, None] == jnp.arange(EXPERTS, dtype=jnp.int32)[None, None, :]).astype(jnp.int32)
    running = jnp.cumsum(onehot, axis=1) - 1
    slots = jnp.sum(onehot * running, axis=2).astype(jnp.int32)
    block_ids = jnp.broadcast_to(jnp.arange(blocks, dtype=jnp.int32)[:, None], (blocks, pairs))
    replica = block_ids % N_DP
    source = block_ids // N_DP
    token_ids = block_ids * TOK_DEV + (jnp.arange(pairs, dtype=jnp.int32) // TOPK)[None, :]
    shape = (N_DP, EXPERTS, N_EXPERT, CAP)
    tables = jnp.full(shape, TOKENS, jnp.int32).at[replica, picks, source, slots].set(token_ids)
    scales = jnp.zeros(shape, jnp.float32).at[replica, picks, source, slots].set(gates.reshape(blocks, pairs))
    zero_row = jnp.zeros((1, D), jnp.bfloat16)
    pad_x = jnp.concatenate([tokens, zero_row], axis=0)
    pad_u = jnp.concatenate([tangent, zero_row], axis=0)
    pad_c = jnp.concatenate([cotangent, zero_row], axis=0)

    def one_expert(carry, expert):
        index = tables[:, expert].reshape(N_DP, -1)
        scale = scales[:, expert].reshape(N_DP, -1)
        rows_x = pad_x[index].astype(jnp.float32)
        rows_u = pad_u[index].astype(jnp.float32)
        rows_dy = rounded(scale[:, :, None] * pad_c[index].astype(jnp.float32))
        w_first = w_in[expert].astype(jnp.float32)
        v_first = v_in[expert].astype(jnp.float32)
        w_second = w_out[expert].astype(jnp.float32)
        v_second = v_out[expert].astype(jnp.float32)
        pre = jnp.einsum("prd,gfd->prgf", rows_x, w_first)
        pre_dot = jnp.einsum("prd,gfd->prgf", rows_u, w_first) + jnp.einsum("prd,gfd->prgf", rows_x, v_first)
        gate_pre, up_val = pre[:, :, 0], pre[:, :, 1]
        gate_dot, up_dot = pre_dot[:, :, 0], pre_dot[:, :, 1]
        back = jnp.einsum("prd,fd->prf", rows_dy, w_second)
        back_dot = jnp.einsum("prd,fd->prf", rows_dy, v_second)
        sigma = jax.nn.sigmoid(gate_pre)
        silu_val = gate_pre * sigma
        first = sigma * (1.0 + gate_pre * (1.0 - sigma))
        second = sigma * (1.0 - sigma) * (2.0 + gate_pre * (1.0 - 2.0 * sigma))
        grad_a = back * up_val * first
        grad_b = back * silu_val
        tang_a = back_dot * up_val * first + back * up_dot * first + back * up_val * second * gate_dot
        tang_b = back_dot * silu_val + back * first * gate_dot
        grads = rounded(jnp.stack([grad_a, grad_b], axis=2))
        tangs = rounded(jnp.stack([tang_a, tang_b], axis=2))
        hidden_dot = rounded(first * gate_dot * up_val + silu_val * up_dot)
        partial_value = jnp.einsum("prgf,gfd->prd", tangs, w_first) + jnp.einsum("prgf,gfd->prd", grads, v_first)
        partial_value = rounded(partial_value)
        carry = carry.at[index.reshape(-1)].add(partial_value.reshape(-1, D))
        part_in = jnp.einsum("prd,prgf->pgfd", rows_u, grads) + jnp.einsum("prd,prgf->pgfd", rows_x, tangs)
        part_out = jnp.einsum("prf,prd->pfd", hidden_dot, rows_dy)
        return carry, (jnp.sum(rounded(part_in), axis=0), jnp.sum(rounded(part_out), axis=0))

    start = jnp.zeros((TOKENS + 1, D), jnp.float32)
    total, results = lax.scan(one_expert, start, jnp.arange(EXPERTS, dtype=jnp.int32))
    return total[:TOKENS], results[0], results[1]
```

```python
import jax
import jax.numpy as jnp
from jax import lax
from jax.sharding import PartitionSpec as P

F32 = jnp.float32
BF16 = jnp.bfloat16
SIDE = 4


def send_x(v, step):
    return lax.ppermute(
        v, "dp", [(p, p // SIDE * SIDE + (p + step) % SIDE) for p in range(SIDE * SIDE)]
    )


def send_y(v, step):
    n = SIDE * SIDE
    return lax.ppermute(v, "dp", [(p, (p + step * SIDE) % n) for p in range(n)])


def send_z(v, step):
    n = lax.axis_size("tensor")
    return lax.ppermute(v, "tensor", [(i, (i + step) % n) for i in range(n)])


def swap_core(v):
    return lax.ppermute(v, "expert", [(0, 1), (1, 0)])


def pick(v, i, axis=0):
    return lax.dynamic_index_in_dim(v, i, axis, keepdims=False)


def ring_gather(v, send):
    half = v.shape[0] // 2
    behind, ahead = send(v, 1), send(v, SIDE - 1)
    low = send(behind[:half], 1)
    high = send(ahead[half:], SIDE - 1)
    return behind, jnp.concatenate([low, high]), ahead


def ring_reduce(blocks, send):
    own, nxt, far, prev = blocks
    half = own.shape[0] // 2
    low = send(far[:half], 1)
    high = send(far[half:], SIDE - 1)
    add = lambda a, b: (a.astype(F32) + b.astype(F32)).astype(BF16)
    up = jnp.concatenate([add(nxt[:half], low), nxt[half:]])
    down = jnp.concatenate([prev[:half], add(prev[half:], high)])
    return own.astype(F32) + send(up, 1).astype(F32) + send(down, SIDE - 1).astype(F32)


def in_order(pieces, me):
    out = jnp.zeros((SIDE, *pieces[0].shape), pieces[0].dtype)
    for s, piece in enumerate(pieces):
        out = lax.dynamic_update_index_in_dim(out, piece, (me - s) % SIDE, 0)
    return out


def dot(a, b, dims):
    return lax.dot_general(a, b, (dims, ((), ())), preferred_element_type=F32)


def split3(w):
    high = lax.reduce_precision(w, 8, 7)
    rest = w - high
    mid = lax.reduce_precision(rest, 8, 7)
    return [high, mid, rest - mid]


def shards(tokens, tangent, cotangent, expert_ids, gates, w_in, v_in, w_out, v_out):
    place = lax.axis_index("dp")
    xi, yi = place % SIDE, place // SIDE
    core, plane = lax.axis_index("expert"), lax.axis_index("tensor")
    n_core, n_plane = lax.axis_size("expert"), lax.axis_size("tensor")
    rows, width = tokens.shape
    hidden, cols = w_in.shape[2], w_in.shape[3]
    part = hidden // SIDE

    stack = jnp.concatenate([w_in[0], v_in[0], w_out, v_out])
    stack = stack.reshape(6, SIDE, part, cols)
    quarters = [pick(stack, xi, 1)]
    quarters += [send_x(pick(stack, (xi + s) % SIDE, 1), s) for s in (1, 2, 3)]
    mine = in_order(quarters, xi)
    behind, far, ahead = ring_gather(mine, send_y)
    whole = in_order([mine, behind, far, ahead], yi)
    whole = whole.reshape(SIDE * SIDE, 6, part, cols)
    whole = jnp.moveaxis(whole, 0, 2).reshape(6, part, width)
    w_a = whole[0:2].reshape(2 * part, width)
    v_a = whole[2:4].reshape(2 * part, width)
    w_o, v_o = whole[4], whole[5]

    marks = []
    for e in range(n_core):
        hit = expert_ids == plane * n_core + e
        marks += split3(jnp.sum(jnp.where(hit, gates, 0.0), axis=1, keepdims=True))
    marks = jnp.concatenate(marks, axis=1)
    marks = jnp.pad(marks, ((0, 0), (0, 128 - marks.shape[1]))).astype(BF16)
    message = jnp.concatenate([tokens, tangent, cotangent, marks], axis=1)
    blocks = [message, *ring_gather(message, send_x)]
    pieces = []
    for block in blocks:
        pieces += [block, swap_core(block)]
    all_rows = jnp.concatenate(pieces)
    rows_x = all_rows[:, :width]
    rows_u = all_rows[:, width : 2 * width]
    marks = all_rows[:, 3 * width :]
    marks = jnp.where(core == 0, marks[:, 0:3], marks[:, 3:6]).astype(F32)
    scale = (marks[:, 0:1] + marks[:, 1:2]) + marks[:, 2:3]
    rows_dy = (scale * all_rows[:, 2 * width : 3 * width].astype(F32)).astype(BF16)

    last = ((1,), (1,))
    pre = dot(rows_x, w_a, last)
    pre_dot = dot(rows_u, w_a, last) + dot(rows_x, v_a, last)
    g, g_dot = dot(rows_dy, w_o, last), dot(rows_dy, v_o, last)
    a, b = pre[:, :part], pre[:, part:]
    a_dot, b_dot = pre_dot[:, :part], pre_dot[:, part:]
    sigma = jax.nn.sigmoid(a)
    s0 = a * sigma
    s1 = sigma * (1.0 + a * (1.0 - sigma))
    s2 = sigma * (1.0 - sigma) * (2.0 + a * (1.0 - 2.0 * sigma))
    grads = jnp.concatenate([g * b * s1, g * s0], axis=1).astype(BF16)
    tang_a = g_dot * b * s1 + g * b_dot * s1 + g * b * s2 * a_dot
    tang_b = g_dot * s0 + g * s1 * a_dot
    tangs = jnp.concatenate([tang_a, tang_b], axis=1).astype(BF16)
    hidden_dot = (s1 * a_dot * b + s0 * b_dot).astype(BF16)

    inner = ((1,), (0,))
    partial = dot(tangs, w_a, inner) + dot(grads, v_a, inner)
    partial = partial.astype(BF16).reshape(SIDE, n_core, rows, width)
    kept = partial[:, 0].astype(F32) + swap_core(partial[:, 1]).astype(F32)
    kept = kept.astype(BF16)
    total = ring_reduce([kept[0], kept[3], kept[2], kept[1]], send_x).astype(BF16)
    lines = total.reshape(n_plane, rows // n_plane, width)
    own = pick(lines, plane).astype(F32)
    for s in (4, 3, 5, 2, 6, 1, 7):
        own = own + send_z(pick(lines, (plane + s) % n_plane), s).astype(F32)
    own = own.astype(BF16)
    out = jnp.zeros(lines.shape, BF16)
    out = lax.dynamic_update_index_in_dim(out, own, plane, 0)
    for s in (4, 3, 5, 2, 6, 1, 7):
        out = lax.dynamic_update_index_in_dim(out, send_z(own, s), (plane - s) % n_plane, 0)
    hvp_tokens = out.reshape(rows, width).astype(F32)

    first = ((0,), (0,))
    part_in = dot(grads, rows_u, first) + dot(tangs, rows_x, first)
    part_out = dot(hidden_dot, rows_dy, first)
    result = jnp.concatenate([part_in, part_out]).astype(BF16)
    result = result.reshape(3 * part, SIDE, SIDE * cols)
    result = ring_reduce([pick(result, (yi + s) % SIDE, 1) for s in range(SIDE)], send_y)
    result = result.astype(BF16).reshape(3 * part, SIDE, cols)
    shares = [pick(result, xi, 1)]
    shares += [send_x(pick(result, (xi + s) % SIDE, 1), s) for s in (1, 2, 3)]
    result = in_order([v.reshape(3, part, cols) for v in shares], xi)
    result = jnp.moveaxis(result, 0, 1).reshape(3, hidden, cols).astype(F32)
    return hvp_tokens, result[None, 0:2], result[2:3]


def solution(mesh):
    row = P(("expert", "dp"), None)
    inward = P(("tensor", "expert"), None, None, "dp")
    outward = P(("tensor", "expert"), None, "dp")
    return jax.shard_map(
        shards,
        mesh=mesh,
        in_specs=(row, row, row, row, row, inward, inward, outward, outward),
        out_specs=(row, inward, outward),
        check_vma=False,
    )
```
